512 devices in a mesh: expert: 128 (over y, z, core), cuts: 4 (over x).
Axes of the slice: x: 4, y: 4, z: 16, core: 2. Of those that a mesh axis runs over, the one named last changes fastest.
Arguments:
- tokens: bfloat16 [1024, 3584], P('expert', 'cuts'), may hold values from -6 to 6
- expert_ids: int32 [1024, 8], P('expert'), may hold values from 0 to 127, all different within a row; in each aligned block of 8 rows (0 to 7, 8 to 15, ...) at most 1 rows name the same one
- gate_weight: float32 [1024, 8], P('expert'), may hold values from 0.05 to 1
- valid_count: int32 [128], P('expert'), may hold values from 6 to 8, as said below
- up_weight: bfloat16 [128, 3584, 1024], P('expert', None, 'cuts'), may hold values from -0.09375 to 0.09375
- down_weight: bfloat16 [128, 1024, 3584], P('expert', 'cuts'), may hold values from -0.1875 to 0.1875
Outputs:
- moe_output: bfloat16 [1024, 3584], P('expert', 'cuts')
The draws below stay inside these ranges and needn't reach their ends.
Inputs may be any that keep to these rules, and one draw needn't show every extreme that they name: `expert_ids`: each row names 8 different experts; within the rows of one group (8 rows) no expert is named more than 1 times, and in some groups one expert is named exactly 1 times. `valid_count`: live tokens of each group, between three quarters of 8 (rounded down) and 8; both ends are reached in every draw.
All inputs are finite; a program needn't handle non-finite values.
Results may differ from the reference program's by a relative error of at most 0.0081.
Values may be sent and summed in bfloat16 or wider, within the bound.
No kernel may reach another device: no remote copies, remote signals or barrier semaphores. Data moves between devices by JAX's collectives and lax.ppermute only.
A program may use at most 64 MiB of HBM per device.

```python
import math
import jax
import jax.numpy as jnp
import numpy as np
from jax import lax

D = 3584
FF = 1024
EXPERTS = 128
TOP = 8
TOK_DEV = 8
CAP = 1
GROUPS = 128
TOKENS = 1024


def draw_valid_count(key, part):
    first_key, second_key = jax.random.split(jax.random.fold_in(key, 7))
    counts = jax.random.randint(first_key, (GROUPS,), 3 * TOK_DEV // 4, TOK_DEV + 1)
    order = jax.random.permutation(second_key, GROUPS)
    counts = counts.at[order[0]].set(TOK_DEV)
    counts = counts.at[order[1]].set(3 * TOK_DEV // 4)
    return counts.astype(jnp.int32)


def block_scale(rng, extent, shards, low, high):
    gain, own = 1.0, jax.random.fold_in(rng, 6)
    for axis_at, blocks in shards:
        heights = jnp.exp(jax.random.uniform(jax.random.fold_in(own, axis_at), (blocks,), jnp.float32, low / len(shards), high / len(shards)))
        gain = gain * jnp.repeat(heights, extent[axis_at] // blocks).reshape([-1 if axis == axis_at else 1 for axis in range(len(extent))])
    return gain


def assign_block(stream_key, own, number, rows, number_of, top, bound, lean):
    order = jax.random.permutation(stream_key, number_of)
    heavy_load, usual = portions_of(number_of, rows * top, bound, lean, True), portions_of(number_of, rows * top, bound, lean, False)
    places = jnp.arange(number_of)

    def named(sizes, offset_by):
        used = int((sizes > 0).sum())
        fixed = max(1, used // 4)
        moved = fixed + (places - fixed + offset_by * (used - fixed)) % max(1, number_of - fixed)
        return jnp.zeros((number_of,), jnp.int32).at[order[jnp.where(places < fixed, places, moved)]].set(jnp.asarray(sizes, jnp.int32))

    sizes = jnp.where(number % 4 == 0, named(heavy_load, number // 4), named(usual, number - number // 4 - 1))
    mixed = jax.random.permutation(jax.random.fold_in(own, 3), number_of)
    giver, receiver = mixed[0:number_of // 2 * 2:2], mixed[1:number_of // 2 * 2:2]
    room = jnp.minimum(sizes[giver] - 1, bound - sizes[receiver]) // 2
    room = jnp.where((giver == order[0]) | (receiver == order[0]) | (sizes[receiver] == 0), 0, jnp.maximum(room, 0))
    moved = jax.random.randint(jax.random.fold_in(own, 4), (number_of // 2,), 0, 1 << 20) % (room + 1)
    sizes = sizes.at[giver].add(-moved).at[receiver].add(moved)
    members = jnp.searchsorted(jnp.cumsum(sizes), jnp.arange(rows * top), side="right").astype(jnp.int32)
    grid = members.reshape(top, rows).T
    grid = grid[jax.random.permutation(jax.random.fold_in(own, 1), rows)]
    offset_by = jax.random.randint(jax.random.fold_in(own, 2), (rows, 1), 0, top)
    return jnp.take_along_axis(grid, (jnp.arange(top)[None, :] + offset_by) % top, axis=1)


def portions_of(amount, total, reach, lean, full):
    loads = [(1 << 20) // math.isqrt(standing ** lean) + 1 for standing in range(1, amount + 1)]
    largest = reach if full else min(reach, max(-(-total // amount), total * loads[0] // sum(loads)))
    least = 1 if total - largest >= amount - 1 else 0
    holding, surplus = [largest] + [least] * (amount - 1), total - largest - least * (amount - 1)
    while surplus > 0:
        free = [i for i in range(1, amount) if holding[i] < largest] or [i for i in range(1, amount) if holding[i] < reach]
        pool, left = sum([loads[i] for i in free]), surplus
        for i in free:
            addition = min(reach - holding[i], max(1, left * loads[i] // pool), surplus)
            holding[i] = holding[i] + addition
            surplus = surplus - addition
    return np.array(holding)


def centred(rng, dims, spread, limit, pieces=(), kind=jnp.bfloat16):
    loudness = block_scale(rng, dims, pieces, -0.22, 0.18) if pieces else 1.0
    array = jax.random.normal(rng, dims, jnp.float32) * spread * loudness
    return jnp.minimum(jnp.maximum(array, -limit), limit).astype(kind)


def setup_inputs(seed: int = 0) -> dict:
    splits = jax.random.split(jax.random.key(seed), 7)
    tokens = centred(splits[0], (TOKENS, D), 1.0, 6.0, ((0, 128), (1, 4)))
    expert_ids_keys = jax.random.split(jax.random.fold_in(splits[1], 1), TOKENS // TOK_DEV)
    expert_ids_turns = jax.random.permutation(jax.random.fold_in(splits[1], 3), TOKENS // TOK_DEV)
    expert_ids = jax.vmap(lambda own, number: assign_block(jax.random.fold_in(splits[1], 2), own, number, TOK_DEV, EXPERTS, TOP, CAP, 2))(expert_ids_keys, expert_ids_turns).reshape((TOKENS, TOP))
    gate_weight = jnp.clip(jnp.exp(math.log(1.0) - 2.9957323 * jax.random.uniform(splits[2], (TOKENS, TOP), jnp.float32) ** block_scale(splits[2], (TOKENS, TOP), ((0, 128),), -0.2, 0.2)), 0.05, 1.0)
    valid_count = draw_valid_count(jax.random.fold_in(splits[6], 71), 0)
    up_weight = centred(splits[4], (EXPERTS, D, FF), D ** -0.5, 0.09375, ((0, 128), (2, 4)))
    down_weight = centred(splits[5], (EXPERTS, FF, D), FF ** -0.5, 0.1875, ((0, 128), (1, 4)))
    return {"tokens": tokens, "expert_ids": expert_ids, "gate_weight": gate_weight, "valid_count": valid_count, "up_weight": up_weight, "down_weight": down_weight}


route_scale = 2.827


def block_tables(expert_rows, gate_rows, count_here):
    tok_rows = expert_rows.shape[0]
    top_rows = expert_rows.shape[1]
    pair_total = tok_rows * top_rows
    flat_ids = expert_rows.reshape(pair_total)
    live_tok = (jnp.arange(tok_rows, dtype=jnp.int32) < count_here).astype(jnp.int32)
    live_pairs = jnp.repeat(live_tok, top_rows)
    expert_hits = (flat_ids[:, None] == jnp.arange(EXPERTS, dtype=jnp.int32)[None, :]).astype(jnp.int32) * live_pairs[:, None]
    earlier = jnp.cumsum(expert_hits, axis=0) - expert_hits
    slot_index = jnp.sum(earlier * expert_hits, axis=1)
    position = flat_ids * CAP + slot_index
    onehot = (position[:, None] == jnp.arange(EXPERTS * CAP, dtype=jnp.int32)[None, :]).astype(jnp.float32)
    onehot = onehot * live_pairs[:, None].astype(jnp.float32)
    onehot = onehot.reshape(tok_rows, top_rows, EXPERTS * CAP)
    shares = route_scale * gate_rows / jnp.sum(gate_rows, axis=1, keepdims=True)
    select = jnp.sum(onehot, axis=1)
    mixing = jnp.einsum('tk,tkp->tp', shares, onehot, precision=lax.Precision.HIGHEST)
    return select, mixing


def reference(tokens, expert_ids, gate_weight, valid_count, up_weight, down_weight):
    groups = valid_count.shape[0]
    tok_blocks = tokens.reshape(groups, TOK_DEV, D)
    id_blocks = expert_ids.reshape(groups, TOK_DEV, TOP)
    gate_blocks = gate_weight.reshape(groups, TOK_DEV, TOP)
    select, mixing = jax.vmap(block_tables)(id_blocks, gate_blocks, valid_count)
    dispatched = jnp.einsum('btp,btd->bpd', select.astype(jnp.float32), tok_blocks.astype(jnp.float32))
    dispatched = dispatched.astype(jnp.bfloat16)
    dispatched = dispatched.reshape(groups, EXPERTS, CAP, D).transpose(1, 0, 2, 3).reshape(EXPERTS, groups * CAP, D)

    def expert(operands):
        rows_in, w_up, w_down = operands
        hidden = jax.nn.silu(jnp.dot(rows_in, w_up, preferred_element_type=jnp.float32)).astype(jnp.bfloat16)
        return jnp.dot(hidden, w_down, preferred_element_type=jnp.float32)

    expert_out = lax.map(expert, (dispatched, up_weight, down_weight))
    expert_out = expert_out.reshape(EXPERTS, groups, CAP, D)
    mixed_rows = jnp.einsum('btec,ebcd->btd', mixing.reshape(groups, TOK_DEV, EXPERTS, CAP), expert_out,
                            precision=lax.Precision.HIGHEST)
    return mixed_rows.reshape(TOKENS, D).astype(jnp.bfloat16)
```

```python
import jax
import jax.numpy as jnp
from jax import lax
from jax.experimental import pallas as pl
from jax.experimental.pallas import tpu as pltpu
from jax.sharding import Mesh, PartitionSpec as P

route_scale = 2.827
Y, ZH, ZL, C, X = 4, 8, 2, 2, 4
NEAR = Y * ZL * C
F32, BF16 = jnp.float32, jnp.bfloat16
VMEM = pl.BlockSpec(memory_space=pltpu.VMEM)
SMEM = pl.BlockSpec(memory_space=pltpu.SMEM)
NOWHERE = 255.0


def pack_kernel(tok_ref, ids_ref, gate_ref, count_ref, out_ref):
    rows, top = ids_ref.shape
    width = tok_ref.shape[1]
    ids = ids_ref[...]
    gate = gate_ref[...]
    share = route_scale * gate / jnp.sum(gate, axis=1, keepdims=True)
    high = share.astype(BF16).astype(F32)
    mid = (share - high).astype(BF16).astype(F32)
    low = (share - high - mid).astype(BF16).astype(F32)
    live = lax.broadcasted_iota(jnp.int32, ids.shape, 0) < count_ref[0]
    near = (ids // (ZH * ZL * C)) * (ZL * C) + ids % (ZL * C)
    near = jnp.where(live, near, int(NOWHERE)).astype(F32)
    far = (ids // (ZL * C)) % ZH
    lane = lax.broadcasted_iota(jnp.int32, (rows, 128), 1)
    meta = jnp.zeros((rows, 128), F32)
    goes = jnp.full((rows, 128), -1, jnp.int32)
    for k in range(top):
        at = slice(k, k + 1)
        meta = jnp.where(lane == k, near[:, at], meta)
        goes = jnp.where(lane == k, far[:, at], goes)
        for piece, part in enumerate((high, mid, low)):
            meta = jnp.where(lane == (piece + 1) * top + k, part[:, at], meta)
    tokens = tok_ref[...]
    for to in range(ZH):
        out_ref[to, :, :width] = tokens
        here = jnp.where((goes == to) | (goes < 0), meta, NOWHERE)
        out_ref[to, :, width:] = here.astype(BF16)


def match_of(meta, top):
    shape = meta.shape
    column = lax.broadcasted_iota(jnp.int32, shape, 1)
    row = lax.broadcasted_iota(jnp.int32, shape, 0)
    own = (row // 8) == (column % ZH)
    expert = jnp.where(own, column // ZH, -1).astype(F32)
    return [meta[:, k : k + 1] == expert for k in range(top)]


def pick_kernel(top, in_ref, out_ref):
    width = out_ref.shape[2]
    rows = in_ref.shape[0] * in_ref.shape[1]
    meta = in_ref[:, :, width:].astype(F32).reshape(rows, 128)
    hits = match_of(meta, top)
    named = hits[0]
    for hit in hits[1:]:
        named = named | hit
    picker = jnp.where(named, 1.0, 0.0).astype(BF16)
    tokens = in_ref[:, :, :width].astype(F32).reshape(rows, width).astype(BF16)
    picked = lax.dot_general(picker, tokens, (((0,), (0,)), ((), ())), preferred_element_type=F32)
    picked = picked.astype(BF16)
    for x in range(X):
        out_ref[x] = picked


def expert_kernel(in_ref, up_ref, down_ref, out_ref):
    width = in_ref.shape[2]
    raised = None
    for x in range(X):
        term = jnp.dot(in_ref[x], up_ref[0, x * width : (x + 1) * width, :], preferred_element_type=F32)
        raised = term if raised is None else raised + term
    hidden = (raised / (1.0 + jnp.exp(-raised))).astype(BF16)
    for x in range(X):
        lowered = jnp.dot(hidden, down_ref[0, :, x * width : (x + 1) * width], preferred_element_type=F32)
        out_ref[x] = lowered.astype(BF16)


def mix_kernel(top, meta_ref, in_ref, out_ref):
    width = in_ref.shape[2]
    rows = meta_ref.shape[0] * meta_ref.shape[1]
    meta = meta_ref[:, :, width:].astype(F32).reshape(rows, 128)
    hits = match_of(meta, top)
    pieces = []
    for piece in range(3):
        weight = jnp.zeros((rows, 128), F32)
        for k in range(top):
            at = (piece + 1) * top + k
            weight = jnp.where(hits[k], meta[:, at : at + 1], weight)
        pieces.append(weight)
    mixing = jnp.concatenate(pieces, axis=0).astype(BF16)
    total = None
    for x in range(X):
        term = jnp.dot(mixing, in_ref[x], preferred_element_type=F32)
        total = term if total is None else total + term
    mixed = (total[2 * rows :] + total[rows : 2 * rows]) + total[:rows]
    out_ref[...] = mixed.astype(BF16)


def call(kernel, out_shape, specs, name, flops, bytes_accessed):
    return pl.pallas_call(
        kernel,
        out_shape=jax.ShapeDtypeStruct(out_shape, BF16),
        in_specs=specs,
        out_specs=VMEM,
        name=name,
        compiler_params=pltpu.CompilerParams(vmem_limit_bytes=16 * 1024 * 1024),
        cost_estimate=pl.CostEstimate(flops=flops, bytes_accessed=bytes_accessed, transcendentals=0),
    )


def shards(tokens, expert_ids, gate_weight, valid_count, up_weight, down_weight):
    rows, width = tokens.shape
    top = expert_ids.shape[1]
    far, near = "zh", ("x", "y", "zl", "c")
    packed = call(pack_kernel, (ZH, rows, width + 128), [VMEM, VMEM, VMEM, SMEM], "pack", 100000, 200000)(
        tokens, expert_ids, gate_weight, valid_count
    )
    got = lax.all_to_all(packed, far, 0, 0, tiled=True)
    slots = NEAR * ZH
    picked = call(lambda *refs: pick_kernel(top, *refs), (X, slots, width), [VMEM], "pick", 2 * 64 * slots * width, 1100000)(got)
    routed = lax.all_to_all(picked.reshape(X * NEAR, ZH, width), near, 0, 0, tiled=True)
    partial = call(expert_kernel, (X, slots, width), [VMEM] * 3, "expert", 4 * slots * X * width * up_weight.shape[2], 5000000)(
        routed.reshape(X, slots, width), up_weight, down_weight
    )
    back = lax.all_to_all(partial.reshape(X * NEAR, ZH, width), near, 0, 0, tiled=True)
    mixed = call(lambda *refs: mix_kernel(top, *refs), (ZH * rows, width), [VMEM] * 2, "mix", 2 * 192 * X * slots * width, 1100000)(
        got, back.reshape(X, slots, width)
    )
    parts = lax.all_to_all(mixed.reshape(ZH, rows, width), far, 0, 0, tiled=True)
    return jnp.sum(parts.astype(F32), axis=0).astype(BF16)


def solution(mesh):
    fine = Mesh(mesh.devices.reshape(Y, ZH, ZL, C, X), ("y", "zh", "zl", "c", "x"))
    experts = ("y", "zh", "zl", "c")
    return jax.shard_map(
        shards,
        mesh=fine,
        in_specs=(
            P(experts, "x"),
            P(experts, None),
            P(experts, None),
            P(experts),
            P(experts, None, "x"),
            P(experts, "x", None),
        ),
        out_specs=P(experts, "x"),
        check_vma=False,
    )
```

```python
import jax
import jax.numpy as jnp
from jax import lax
from jax.experimental import pallas as pl
from jax.experimental.pallas import tpu as pltpu
from jax.sharding import Mesh, PartitionSpec as P

route_scale = 2.827
Y, ZH, ZL, C, X = 4, 8, 2, 2, 4
NEAR = Y * ZL * C
F32, BF16 = jnp.float32, jnp.bfloat16
VMEM = pl.BlockSpec(memory_space=pltpu.VMEM)
SMEM = pl.BlockSpec(memory_space=pltpu.SMEM)
HBM = pl.BlockSpec(memory_space=pltpu.HBM)
NOWHERE = 255.0
ZH_OF = (0, 4, 2, 6, 1, 5, 3, 7)


def pack_kernel(tok_hbm, ids_hbm, gate_hbm, count_ref, out_ref, tok_ref, ids_ref, gate_ref, sems):
    pairs = ((ids_hbm, ids_ref), (gate_hbm, gate_ref), (tok_hbm, tok_ref))
    copies = [pltpu.make_async_copy(src, dst, sems.at[i]) for i, (src, dst) in enumerate(pairs)]
    for copy in copies:
        copy.start()
    for copy in copies[:2]:
        copy.wait()
    rows, top = ids_ref.shape
    width = tok_ref.shape[1]
    ids = ids_ref[...]
    gate = gate_ref[...]
    share = route_scale * gate / jnp.sum(gate, axis=1, keepdims=True)
    high = share.astype(BF16).astype(F32)
    mid = (share - high).astype(BF16).astype(F32)
    low = (share - high - mid).astype(BF16).astype(F32)
    live = lax.broadcasted_iota(jnp.int32, ids.shape, 0) < count_ref[0]
    near = (ids // (ZH * ZL * C)) * (ZL * C) + ids % (ZL * C)
    near = jnp.where(live, near, int(NOWHERE)).astype(F32)
    far = (ids // (ZL * C)) % ZH
    lane = lax.broadcasted_iota(jnp.int32, (rows, 128), 1)
    meta = jnp.zeros((rows, 128), F32)
    goes = jnp.full((rows, 128), -1, jnp.int32)
    for k in range(top):
        at = slice(k, k + 1)
        meta = jnp.where(lane == k, near[:, at], meta)
        goes = jnp.where(lane == k, far[:, at], goes)
        for piece, part in enumerate((high, mid, low)):
            meta = jnp.where(lane == (piece + 1) * top + k, part[:, at], meta)
    for to in range(ZH):
        here = jnp.where((goes == ZH_OF[to]) | (goes < 0), meta, NOWHERE)
        out_ref[to, :, width:] = here.astype(BF16)
    copies[2].wait()
    tokens = tok_ref[...]
    for to in range(ZH):
        out_ref[to, :, :width] = tokens


def match_of(meta, top):
    shape = meta.shape
    column = lax.broadcasted_iota(jnp.int32, shape, 1)
    row = lax.broadcasted_iota(jnp.int32, shape, 0)
    own = (row // 8) == (column % ZH)
    expert = jnp.where(own, column // ZH, -1).astype(F32)
    return [meta[:, k : k + 1] == expert for k in range(top)]


def pick_kernel(top, in_ref, out_ref):
    width = out_ref.shape[2]
    rows = in_ref.shape[0] * in_ref.shape[1]
    meta = in_ref[:, :, width:].astype(F32).reshape(rows, 128)
    hits = match_of(meta, top)
    named = hits[0]
    for hit in hits[1:]:
        named = named | hit
    picker = jnp.where(named, 1.0, 0.0).astype(BF16)
    tokens = in_ref[:, :, :width].astype(F32).reshape(rows, width).astype(BF16)
    picked = lax.dot_general(picker, tokens, (((0,), (0,)), ((), ())), preferred_element_type=F32)
    picked = picked.astype(BF16)
    for x in range(X):
        out_ref[x] = picked


def expert_kernel(in_ref, up_ref, down_ref, out_ref):
    width = in_ref.shape[2]
    raised = None
    for x in range(X):
        term = jnp.dot(in_ref[x], up_ref[0, x * width : (x + 1) * width, :], preferred_element_type=F32)
        raised = term if raised is None else raised + term
    hidden = (raised / (1.0 + jnp.exp(-raised))).astype(BF16)
    for x in range(X):
        lowered = jnp.dot(hidden, down_ref[0, :, x * width : (x + 1) * width], preferred_element_type=F32)
        out_ref[x] = lowered.astype(BF16)


def mix_kernel(top, meta_ref, in_ref, out_ref):
    width = in_ref.shape[2]
    rows = meta_ref.shape[0] * meta_ref.shape[1]
    meta = meta_ref[:, :, width:].astype(F32).reshape(rows, 128)
    hits = match_of(meta, top)
    pieces = []
    for piece in range(3):
        weight = jnp.zeros((rows, 128), F32)
        for k in range(top):
            at = (piece + 1) * top + k
            weight = jnp.where(hits[k], meta[:, at : at + 1], weight)
        pieces.append(weight)
    mixing = jnp.concatenate(pieces, axis=0).astype(BF16)
    total = None
    for x in range(X):
        term = jnp.dot(mixing, in_ref[x], preferred_element_type=F32)
        total = term if total is None else total + term
    mixed = (total[2 * rows :] + total[rows : 2 * rows]) + total[:rows]
    out_ref[...] = mixed.astype(BF16)


def call(kernel, out_shape, specs, name, flops, bytes_accessed, scratch=()):
    return pl.pallas_call(
        kernel,
        out_shape=jax.ShapeDtypeStruct(out_shape, BF16),
        in_specs=specs,
        out_specs=VMEM,
        scratch_shapes=list(scratch),
        name=name,
        compiler_params=pltpu.CompilerParams(vmem_limit_bytes=16 * 1024 * 1024),
        cost_estimate=pl.CostEstimate(flops=flops, bytes_accessed=bytes_accessed, transcendentals=0),
    )


def in_hbm(array):
    return pltpu.with_memory_space_constraint(array, pltpu.HBM)


def shards(tokens, expert_ids, gate_weight, valid_count, up_weight, down_weight):
    rows, width = tokens.shape
    top = expert_ids.shape[1]
    hidden = up_weight.shape[2]
    far, near = ("zd", "zb", "za"), ("x", "y", "zl", "c")
    slots = NEAR * ZH
    packed = call(
        pack_kernel,
        (ZH, rows, width + 128),
        [HBM] * 3 + [SMEM],
        "pack",
        100000,
        200000,
        [
            pltpu.VMEM(tokens.shape, BF16),
            pltpu.VMEM(expert_ids.shape, jnp.int32),
            pltpu.VMEM(gate_weight.shape, F32),
            pltpu.SemaphoreType.DMA((3,)),
        ],
    )(in_hbm(tokens), in_hbm(expert_ids), in_hbm(gate_weight), valid_count)
    got = lax.all_to_all(packed, far, 0, 0, tiled=True)
    picked = call(
        lambda *refs: pick_kernel(top, *refs), (X, slots, width), [VMEM], "pick", 4 * 10**9, 1100000
    )(got)
    routed = lax.all_to_all(picked.reshape(X * NEAR, ZH, width), near, 0, 0, tiled=True)
    partial = call(
        expert_kernel,
        (X, slots, width),
        [VMEM] * 3,
        "expert",
        4 * slots * X * width * hidden,
        5000000,
    )(routed.reshape(X, slots, width), up_weight, down_weight)
    back = lax.all_to_all(partial.reshape(X * NEAR, ZH, width), near, 0, 0, tiled=True)
    mixed = call(
        lambda *refs: mix_kernel(top, *refs), (ZH * rows, width), [VMEM] * 2, "mix", 2 * 192 * X * slots * width, 1100000
    )(got, back.reshape(X, slots, width))
    parts = lax.all_to_all(mixed.reshape(ZH, rows, width), far, 0, 0, tiled=True)
    return jnp.sum(parts.astype(F32), axis=0).astype(BF16)


def solution(mesh):
    fine = Mesh(mesh.devices.reshape(Y, 2, 2, 2, ZL, C, X), ("y", "za", "zb", "zd", "zl", "c", "x"))
    experts = ("y", "za", "zb", "zd", "zl", "c")
    return jax.shard_map(
        shards,
        mesh=fine,
        in_specs=(
            P(experts, "x"),
            P(experts, None),
            P(experts, None),
            P(experts),
            P(experts, None, "x"),
            P(experts, "x", None),
        ),
        out_specs=P(experts, "x"),
        check_vma=False,
    )
```

```python
import jax
import jax.numpy as jnp
from jax import lax
from jax.experimental import pallas as pl
from jax.experimental.pallas import tpu as pltpu
from jax.sharding import Mesh, PartitionSpec as P

route_scale = 2.827
Y, ZH, ZL, C, X = 4, 8, 2, 2, 4
F32, BF16 = jnp.float32, jnp.bfloat16
VMEM = pl.BlockSpec(memory_space=pltpu.VMEM)
SMEM = pl.BlockSpec(memory_space=pltpu.SMEM)
HBM = pl.BlockSpec(memory_space=pltpu.HBM)
NOWHERE = 255.0
ZH_OF = (0, 4, 2, 6, 1, 5, 3, 7)


def pack_kernel(tok_hbm, ids_hbm, gate_hbm, count_ref, out_ref, tok_ref, ids_ref, gate_ref, sems):
    pairs = ((ids_hbm, ids_ref), (gate_hbm, gate_ref), (tok_hbm, tok_ref))
    copies = [pltpu.make_async_copy(src, dst, sems.at[i]) for i, (src, dst) in enumerate(pairs)]
    for copy in copies:
        copy.start()
    for copy in copies[:2]:
        copy.wait()
    rows, top = ids_ref.shape
    width = tok_ref.shape[1]
    ids = ids_ref[...]
    gate = gate_ref[...]
    share = route_scale * gate / jnp.sum(gate, axis=1, keepdims=True)
    high = share.astype(BF16).astype(F32)
    mid = (share - high).astype(BF16).astype(F32)
    low = (share - high - mid).astype(BF16).astype(F32)
    live = lax.broadcasted_iota(jnp.int32, ids.shape, 0) < count_ref[0]
    names = jnp.where(live, ids, int(NOWHERE)).astype(F32)
    lane = lax.broadcasted_iota(jnp.int32, (rows, 128), 1)
    meta = jnp.zeros((rows, 128), F32)
    for k in range(top):
        at = slice(k, k + 1)
        for piece, part in enumerate((names, high, mid, low)):
            meta = jnp.where(lane == piece * top + k, part[:, at], meta)
    out_ref[:, width:] = meta.astype(BF16)
    copies[2].wait()
    out_ref[:, :width] = tok_ref[...]


def pick_kernel(top, in_ref, out_ref):
    width = out_ref.shape[2]
    rows = ZH * C * in_ref.shape[2]
    meta = in_ref[:, :, :, width:].astype(F32).reshape(rows, 128)
    column = lax.broadcasted_iota(jnp.int32, (rows, 128), 1)
    row = lax.broadcasted_iota(jnp.int32, (rows, 128), 0)
    own = (row // (8 * C) == column % ZH) & ((row // 8) % C == (column // ZH) % C)
    near = column // (ZH * C)
    expert = ((near // ZL) * ZH + lax.axis_index(("za", "zb", "zd"))) * (ZL * C) + (near % ZL) * C + lax.axis_index("c")
    expert = jnp.where(own, expert, -1).astype(F32)
    named = meta[:, 0:1] == expert
    for k in range(1, top):
        named = named | (meta[:, k : k + 1] == expert)
    picker = jnp.where(named, 1.0, 0.0).astype(BF16)
    tokens = in_ref[:, :, :, :width].astype(F32).reshape(rows, width).astype(BF16)
    picked = lax.dot_general(picker, tokens, (((0,), (0,)), ((), ())), preferred_element_type=F32)
    picked = picked.astype(BF16)
    for x in range(X):
        out_ref[x] = picked


def mixing_of(top, meta):
    column = lax.broadcasted_iota(jnp.int32, meta.shape, 1)
    row = lax.broadcasted_iota(jnp.int32, meta.shape, 0)
    near = column // ZH
    expert = ((near // (ZL * C)) * ZH + lax.axis_index(("za", "zb", "zd"))) * (ZL * C) + near % (ZL * C)
    expert = jnp.where(row // 8 == column % ZH, expert, -1).astype(F32)
    hits = [meta[:, k : k + 1] == expert for k in range(top)]
    pieces = []
    for piece in range(3):
        weight = jnp.zeros(meta.shape, F32)
        for k in range(top):
            at = (piece + 1) * top + k
            weight = jnp.where(hits[k], meta[:, at : at + 1], weight)
        pieces.append(weight.astype(BF16))
    return pieces


def expert_kernel(top, in_ref, up_ref, down_ref, meta_ref, out_ref, mixing_ref):
    width = in_ref.shape[2]
    raised = None
    for x in range(X):
        term = jnp.dot(in_ref[x], up_ref[0, x * width : (x + 1) * width, :], preferred_element_type=F32)
        raised = term if raised is None else raised + term
    rows = ZH * meta_ref.shape[2]
    meta = meta_ref[:, lax.axis_index("c"), :, width:].astype(F32).reshape(rows, 128)
    for piece, weight in enumerate(mixing_of(top, meta)):
        mixing_ref[piece * rows : (piece + 1) * rows] = weight
    hidden = (raised / (1.0 + jnp.exp(-raised))).astype(BF16)
    for x in range(X):
        lowered = jnp.dot(hidden, down_ref[0, :, x * width : (x + 1) * width], preferred_element_type=F32)
        out_ref[x] = lowered.astype(BF16)


def mix_kernel(mixing_ref, in_ref, out_ref):
    rows = mixing_ref.shape[0] // 3
    total = None
    for x in range(X):
        term = jnp.dot(mixing_ref[...], in_ref[x], preferred_element_type=F32)
        total = term if total is None else total + term
    mixed = (total[2 * rows :] + total[rows : 2 * rows]) + total[:rows]
    for to in range(ZH):
        out_ref[to] = mixed[ZH_OF[to] * 8 : ZH_OF[to] * 8 + 8].astype(BF16)


def call(kernel, out_shape, specs, name, flops, bytes_accessed, scratch=()):
    return pl.pallas_call(
        kernel,
        out_shape=[jax.ShapeDtypeStruct(shape, BF16) for shape in out_shape],
        in_specs=specs,
        out_specs=[VMEM] * len(out_shape),
        scratch_shapes=list(scratch),
        name=name,
        compiler_params=pltpu.CompilerParams(vmem_limit_bytes=16 * 1024 * 1024),
        cost_estimate=pl.CostEstimate(flops=flops, bytes_accessed=bytes_accessed, transcendentals=0),
    )


def in_hbm(array):
    return pltpu.with_memory_space_constraint(array, pltpu.HBM)


def shards(tokens, expert_ids, gate_weight, valid_count, up_weight, down_weight):
    rows, width = tokens.shape
    top = expert_ids.shape[1]
    hidden = up_weight.shape[2]
    far, near = ("zd", "zb", "za"), ("x", "y", "zl")
    slots = Y * ZL * C * ZH
    (packed,) = call(
        pack_kernel,
        [(rows, width + 128)],
        [HBM] * 3 + [SMEM],
        "pack",
        100000,
        200000,
        [
            pltpu.VMEM(tokens.shape, BF16),
            pltpu.VMEM(expert_ids.shape, jnp.int32),
            pltpu.VMEM(gate_weight.shape, F32),
            pltpu.SemaphoreType.DMA((3,)),
        ],
    )(in_hbm(tokens), in_hbm(expert_ids), in_hbm(gate_weight), valid_count)
    got = lax.all_gather(packed, ("za", "zb", "zd", "c"), axis=0, tiled=False).reshape(ZH, C, rows, width + 128)
    (picked,) = call(lambda *refs: pick_kernel(top, *refs), [(X, slots, width)], [VMEM], "pick", 4 * 10**9, 1100000)(got)
    routed = lax.all_to_all(picked.reshape(X * Y * ZL, C * ZH, width), near, 0, 0, tiled=True)
    partial, mixing = call(
        lambda *refs: expert_kernel(top, *refs),
        [(X, slots, width), (3 * ZH * rows, slots)],
        [VMEM] * 4,
        "expert",
        4 * slots * X * width * hidden,
        5000000,
    )(routed.reshape(X, slots, width), up_weight, down_weight, got)
    back = lax.all_to_all(partial.reshape(X * Y * ZL * C, ZH, width), near + ("c",), 0, 0, tiled=True)
    (mixed,) = call(mix_kernel, [(ZH, rows, width)], [VMEM] * 2, "mix", 6 * ZH * rows * X * slots * width, 1100000)(
        mixing, back.reshape(X, slots, width)
    )
    parts = lax.all_to_all(mixed, far, 0, 0, tiled=True)
    return jnp.sum(parts.astype(F32), axis=0).astype(BF16)


def solution(mesh):
    fine = Mesh(mesh.devices.reshape(Y, 2, 2, 2, ZL, C, X), ("y", "za", "zb", "zd", "zl", "c", "x"))
    experts = ("y", "za", "zb", "zd", "zl", "c")
    return jax.shard_map(
        shards,
        mesh=fine,
        in_specs=(
            P(experts, "x"),
            P(experts, None),
            P(experts, None),
            P(experts),
            P(experts, None, "x"),
            P(experts, "x", None),
        ),
        out_specs=P(experts, "x"),
        check_vma=False,
    )
```

```python
import jax
import jax.numpy as jnp
from jax import lax
from jax.experimental import pallas as pl
from jax.experimental.pallas import tpu as pltpu
from jax.sharding import Mesh, PartitionSpec as P

route_scale = 2.827
Y, ZH, ZL, C, X = 4, 8, 2, 2, 4
F32, BF16 = jnp.float32, jnp.bfloat16
VMEM = pl.BlockSpec(memory_space=pltpu.VMEM)
SMEM = pl.BlockSpec(memory_space=pltpu.SMEM)
HBM = pl.BlockSpec(memory_space=pltpu.HBM)
NOWHERE = 255.0
ZH_OF = (0, 4, 2, 6, 1, 5, 3, 7)


def pack_kernel(tok_hbm, ids_hbm, gate_hbm, count_ref, out_ref, tok_ref, ids_ref, gate_ref, sems):
    pairs = ((ids_hbm, ids_ref), (gate_hbm, gate_ref), (tok_hbm, tok_ref))
    copies = [pltpu.make_async_copy(src, dst, sems.at[i]) for i, (src, dst) in enumerate(pairs)]
    for copy in copies:
        copy.start()
    for copy in copies[:2]:
        copy.wait()
    rows, top = ids_ref.shape
    width = tok_ref.shape[1]
    ids = ids_ref[...]
    gate = gate_ref[...]
    high = gate.astype(BF16).astype(F32)
    mid = (gate - high).astype(BF16).astype(F32)
    low = (gate - high - mid).astype(BF16).astype(F32)
    live = lax.broadcasted_iota(jnp.int32, ids.shape, 0) < count_ref[0]
    names = jnp.where(live, ids, int(NOWHERE)).astype(F32)
    lane = lax.broadcasted_iota(jnp.int32, (rows, 128), 1)
    meta = jnp.zeros((rows, 128), F32)
    for k in range(top):
        at = slice(k, k + 1)
        for piece, part in enumerate((names, high, mid, low)):
            meta = jnp.where(lane == piece * top + k, part[:, at], meta)
    out_ref[:, width:] = meta.astype(BF16)
    copies[2].wait()
    out_ref[:, :width] = tok_ref[...]


def pick_kernel(top, in_ref, out_ref):
    width = out_ref.shape[2]
    rows = ZH * C * in_ref.shape[2]
    meta = in_ref[:, :, :, width:].astype(F32).reshape(rows, 128)
    column = lax.broadcasted_iota(jnp.int32, (rows, 128), 1)
    row = lax.broadcasted_iota(jnp.int32, (rows, 128), 0)
    own = (row // (8 * C) == column % ZH) & ((row // 8) % C == (column // ZH) % C)
    near = column // (ZH * C)
    expert = ((near // ZL) * ZH + lax.axis_index(("za", "zb", "zd"))) * (ZL * C) + (near % ZL) * C + lax.axis_index("c")
    expert = jnp.where(own, expert, -1).astype(F32)
    named = meta[:, 0:1] == expert
    for k in range(1, top):
        named = named | (meta[:, k : k + 1] == expert)
    picker = jnp.where(named, 1.0, 0.0).astype(BF16)
    tokens = in_ref[:, :, :, :width].astype(F32).reshape(rows, width).astype(BF16)
    picked = lax.dot_general(picker, tokens, (((0,), (0,)), ((), ())), preferred_element_type=F32)
    picked = picked.astype(BF16)
    for x in range(X):
        out_ref[x] = picked


def mixing_of(top, meta):
    column = lax.broadcasted_iota(jnp.int32, meta.shape, 1)
    row = lax.broadcasted_iota(jnp.int32, meta.shape, 0)
    near = column // ZH
    expert = ((near // (ZL * C)) * ZH + lax.axis_index(("za", "zb", "zd"))) * (ZL * C) + near % (ZL * C)
    expert = jnp.where(row // 8 == column % ZH, expert, -1).astype(F32)
    hits = [meta[:, k : k + 1] == expert for k in range(top)]
    total = jnp.zeros((meta.shape[0], 1), F32)
    weight = jnp.zeros(meta.shape, F32)
    for k in range(top):
        high, mid, low = (meta[:, (piece + 1) * top + k : (piece + 1) * top + k + 1] for piece in range(3))
        gate = (high + mid) + low
        total = total + gate
        weight = jnp.where(hits[k], gate, weight)
    share = route_scale * weight / total
    high = share.astype(BF16)
    mid = (share - high.astype(F32)).astype(BF16)
    low = (share - high.astype(F32) - mid.astype(F32)).astype(BF16)
    return [high, mid, low]


def expert_kernel(top, in_ref, up_ref, down_ref, meta_ref, out_ref, mixing_ref):
    width = in_ref.shape[2]
    raised = None
    for x in range(X):
        term = jnp.dot(in_ref[x], up_ref[0, x * width : (x + 1) * width, :], preferred_element_type=F32)
        raised = term if raised is None else raised + term
    rows = ZH * meta_ref.shape[2]
    meta = meta_ref[:, lax.axis_index("c"), :, width:].astype(F32).reshape(rows, 128)
    for piece, weight in enumerate(mixing_of(top, meta)):
        mixing_ref[piece * rows : (piece + 1) * rows] = weight
    hidden = (raised / (1.0 + jnp.exp(-raised))).astype(BF16)
    for x in range(X):
        lowered = jnp.dot(hidden, down_ref[0, :, x * width : (x + 1) * width], preferred_element_type=F32)
        out_ref[x] = lowered.astype(BF16)


def mix_kernel(mixing_ref, in_ref, out_ref):
    rows = mixing_ref.shape[0] // 3
    total = None
    for x in range(X):
        term = jnp.dot(mixing_ref[...], in_ref[x], preferred_element_type=F32)
        total = term if total is None else total + term
    mixed = (total[2 * rows :] + total[rows : 2 * rows]) + total[:rows]
    for to in range(ZH):
        out_ref[to] = mixed[ZH_OF[to] * 8 : ZH_OF[to] * 8 + 8].astype(BF16)


def call(kernel, out_shape, specs, name, flops, bytes_accessed, scratch=()):
    return pl.pallas_call(
        kernel,
        out_shape=[jax.ShapeDtypeStruct(shape, BF16) for shape in out_shape],
        in_specs=specs,
        out_specs=[VMEM] * len(out_shape),
        scratch_shapes=list(scratch),
        name=name,
        compiler_params=pltpu.CompilerParams(vmem_limit_bytes=16 * 1024 * 1024),
        cost_estimate=pl.CostEstimate(flops=flops, bytes_accessed=bytes_accessed, transcendentals=0),
    )


def in_hbm(array):
    return pltpu.with_memory_space_constraint(array, pltpu.HBM)


def shards(tokens, expert_ids, gate_weight, valid_count, up_weight, down_weight):
    rows, width = tokens.shape
    top = expert_ids.shape[1]
    hidden = up_weight.shape[2]
    far, near = ("zd", "zb", "za"), ("x", "y", "zl")
    slots = Y * ZL * C * ZH
    (packed,) = call(
        pack_kernel,
        [(rows, width + 128)],
        [HBM] * 3 + [SMEM],
        "pack",
        100000,
        200000,
        [
            pltpu.VMEM(tokens.shape, BF16),
            pltpu.VMEM(expert_ids.shape, jnp.int32),
            pltpu.VMEM(gate_weight.shape, F32),
            pltpu.SemaphoreType.DMA((3,)),
        ],
    )(in_hbm(tokens), in_hbm(expert_ids), in_hbm(gate_weight), valid_count)
    got = lax.all_gather(packed, ("za", "zb", "zd", "c"), axis=0, tiled=False).reshape(ZH, C, rows, width + 128)
    (picked,) = call(lambda *refs: pick_kernel(top, *refs), [(X, slots, width)], [VMEM], "pick", 4 * 10**9, 1100000)(got)
    routed = lax.all_to_all(picked.reshape(X * Y * ZL, C * ZH, width), near, 0, 0, tiled=True)
    partial, mixing = call(
        lambda *refs: expert_kernel(top, *refs),
        [(X, slots, width), (3 * ZH * rows, slots)],
        [VMEM] * 4,
        "expert",
        4 * slots * X * width * hidden,
        5000000,
    )(routed.reshape(X, slots, width), up_weight, down_weight, got)
    back = lax.all_to_all(partial.reshape(X * Y * ZL * C, ZH, width), near + ("c",), 0, 0, tiled=True)
    (mixed,) = call(mix_kernel, [(ZH, rows, width)], [VMEM] * 2, "mix", 6 * ZH * rows * X * slots * width, 1100000)(
        mixing, back.reshape(X, slots, width)
    )
    parts = lax.all_to_all(mixed, far, 0, 0, tiled=True)
    return jnp.sum(parts.astype(F32), axis=0).astype(BF16)


def solution(mesh):
    fine = Mesh(mesh.devices.reshape(Y, 2, 2, 2, ZL, C, X), ("y", "za", "zb", "zd", "zl", "c", "x"))
    experts = ("y", "za", "zb", "zd", "zl", "c")
    return jax.shard_map(
        shards,
        mesh=fine,
        in_specs=(
            P(experts, "x"),
            P(experts, None),
            P(experts, None),
            P(experts),
            P(experts, None, "x"),
            P(experts, "x", None),
        ),
        out_specs=P(experts, "x"),
        check_vma=False,
    )
```

```python
import jax
import jax.numpy as jnp
from jax import lax
from jax.experimental import pallas as pl
from jax.experimental.pallas import tpu as pltpu
from jax.sharding import Mesh, PartitionSpec as P

route_scale = 2.827
Y, ZH, ZL, C, X = 4, 8, 2, 2, 4
F32, BF16 = jnp.float32, jnp.bfloat16
VMEM = pl.BlockSpec(memory_space=pltpu.VMEM)
SMEM = pl.BlockSpec(memory_space=pltpu.SMEM)
HBM = pl.BlockSpec(memory_space=pltpu.HBM)
NOWHERE = 255.0
ZH_OF = (0, 4, 2, 6, 1, 5, 3, 7)


def pack_kernel(tok_hbm, ids_hbm, gate_hbm, count_ref, out_ref, tok_ref, ids_ref, gate_ref, sems):
    pairs = ((ids_hbm, ids_ref), (gate_hbm, gate_ref), (tok_hbm, tok_ref))
    copies = [pltpu.make_async_copy(src, dst, sems.at[i]) for i, (src, dst) in enumerate(pairs)]
    for copy in copies:
        copy.start()
    for copy in copies[:2]:
        copy.wait()
    rows, top = ids_ref.shape
    width = tok_ref.shape[1]
    ids = ids_ref[...]
    gate = gate_ref[...]
    high = gate.astype(BF16).astype(F32)
    mid = (gate - high).astype(BF16).astype(F32)
    low = (gate - high - mid).astype(BF16).astype(F32)
    live = lax.broadcasted_iota(jnp.int32, ids.shape, 0) < count_ref[0]
    names = jnp.where(live, ids, int(NOWHERE)).astype(F32)
    lane = lax.broadcasted_iota(jnp.int32, (rows, 128), 1)
    meta = jnp.zeros((rows, 128), F32)
    for k in range(top):
        at = slice(k, k + 1)
        for piece, part in enumerate((names, high, mid, low)):
            meta = jnp.where(lane == piece * top + k, part[:, at], meta)
    out_ref[:, width:] = meta.astype(BF16)
    copies[2].wait()
    out_ref[:, :width] = tok_ref[...]


def pick_kernel(top, in_ref, out_ref):
    width = out_ref.shape[2]
    rows = ZH * C * in_ref.shape[2]
    meta = in_ref[:, :, :, width:].astype(F32).reshape(rows, 128)
    column = lax.broadcasted_iota(jnp.int32, (rows, 128), 1)
    row = lax.broadcasted_iota(jnp.int32, (rows, 128), 0)
    own = (row // (8 * C) == column % ZH) & ((row // 8) % C == (column // ZH) % C)
    near = column // (ZH * C)
    expert = ((near // ZL) * ZH + lax.axis_index(("za", "zb", "zd"))) * (ZL * C) + (near % ZL) * C + lax.axis_index("c")
    expert = jnp.where(own, expert, -1).astype(F32)
    named = meta[:, 0:1] == expert
    for k in range(1, top):
        named = named | (meta[:, k : k + 1] == expert)
    picker = jnp.where(named, 1.0, 0.0).astype(BF16)
    tokens = in_ref[:, :, :, :width].astype(F32).reshape(rows, width).astype(BF16)
    picked = lax.dot_general(picker, tokens, (((0,), (0,)), ((), ())), preferred_element_type=F32)
    picked = picked.astype(BF16)
    for x in range(X):
        out_ref[x] = picked


def mixing_of(top, meta):
    column = lax.broadcasted_iota(jnp.int32, meta.shape, 1)
    row = lax.broadcasted_iota(jnp.int32, meta.shape, 0)
    near = column // ZH
    expert = ((near // (ZL * C)) * ZH + lax.axis_index(("za", "zb", "zd"))) * (ZL * C) + near % (ZL * C)
    expert = jnp.where(row // 8 == column % ZH, expert, -1).astype(F32)
    hits = [meta[:, k : k + 1] == expert for k in range(top)]
    total = jnp.zeros((meta.shape[0], 1), F32)
    weight = jnp.zeros(meta.shape, F32)
    for k in range(top):
        high, mid, low = (meta[:, (piece + 1) * top + k : (piece + 1) * top + k + 1] for piece in range(3))
        gate = (high + mid) + low
        total = total + gate
        weight = jnp.where(hits[k], gate, weight)
    share = route_scale * weight / total
    high = share.astype(BF16)
    mid = (share - high.astype(F32)).astype(BF16)
    low = (share - high.astype(F32) - mid.astype(F32)).astype(BF16)
    return [high, mid, low]


def expert_kernel(top, in_ref, up_ref, down_ref, meta_ref, out_ref, mixing_ref):
    width = in_ref.shape[2]
    raised = None
    for x in range(X):
        term = jnp.dot(in_ref[x], up_ref[0, x * width : (x + 1) * width, :], preferred_element_type=F32)
        raised = term if raised is None else raised + term
    rows = ZH * meta_ref.shape[2]
    meta = meta_ref[:, lax.axis_index("c"), :, width:].astype(F32).reshape(rows, 128)
    for piece, weight in enumerate(mixing_of(top, meta)):
        mixing_ref[piece * rows : (piece + 1) * rows] = weight
    hidden = (raised / (1.0 + jnp.exp(-raised))).astype(BF16)
    for x in range(X):
        lowered = jnp.dot(hidden, down_ref[0, :, x * width : (x + 1) * width], preferred_element_type=F32)
        out_ref[x] = lowered.astype(BF16)


def mix_kernel(mixing_ref, in_ref, out_ref):
    rows = mixing_ref.shape[0] // 3
    twice = jnp.concatenate([mixing_ref[...]] * 2, axis=1)
    slots, width = in_ref.shape[1:]
    total = None
    for x in range(0, X, 2):
        pair = in_ref[x : x + 2].reshape(2 * slots, width)
        term = jnp.dot(twice, pair, preferred_element_type=F32)
        total = term if total is None else total + term
    mixed = (total[2 * rows :] + total[rows : 2 * rows]) + total[:rows]
    for to in range(ZH):
        out_ref[to] = mixed[ZH_OF[to] * 8 : ZH_OF[to] * 8 + 8].astype(BF16)


def call(kernel, out_shape, specs, name, flops, bytes_accessed, scratch=()):
    return pl.pallas_call(
        kernel,
        out_shape=[jax.ShapeDtypeStruct(shape, BF16) for shape in out_shape],
        in_specs=specs,
        out_specs=[VMEM] * len(out_shape),
        scratch_shapes=list(scratch),
        name=name,
        compiler_params=pltpu.CompilerParams(vmem_limit_bytes=16 * 1024 * 1024),
        cost_estimate=pl.CostEstimate(flops=flops, bytes_accessed=bytes_accessed, transcendentals=0),
    )


def in_hbm(array):
    return pltpu.with_memory_space_constraint(array, pltpu.HBM)


def shards(tokens, expert_ids, gate_weight, valid_count, up_weight, down_weight):
    rows, width = tokens.shape
    top = expert_ids.shape[1]
    hidden = up_weight.shape[2]
    far, near = ("zd", "zb", "za"), ("x", "y", "zl")
    slots = Y * ZL * C * ZH
    (packed,) = call(
        pack_kernel,
        [(rows, width + 128)],
        [HBM] * 3 + [SMEM],
        "pack",
        100000,
        200000,
        [
            pltpu.VMEM(tokens.shape, BF16),
            pltpu.VMEM(expert_ids.shape, jnp.int32),
            pltpu.VMEM(gate_weight.shape, F32),
            pltpu.SemaphoreType.DMA((3,)),
        ],
    )(in_hbm(tokens), in_hbm(expert_ids), in_hbm(gate_weight), valid_count)
    got = lax.all_gather(packed, ("za", "zb", "zd", "c"), axis=0, tiled=False).reshape(ZH, C, rows, width + 128)
    (picked,) = call(lambda *refs: pick_kernel(top, *refs), [(X, slots, width)], [VMEM], "pick", 4 * 10**9, 1100000)(got)
    routed = lax.all_to_all(picked.reshape(X * Y * ZL, C * ZH, width), near, 0, 0, tiled=True)
    partial, mixing = call(
        lambda *refs: expert_kernel(top, *refs),
        [(X, slots, width), (3 * ZH * rows, slots)],
        [VMEM] * 4,
        "expert",
        4 * slots * X * width * hidden,
        5000000,
    )(routed.reshape(X, slots, width), up_weight, down_weight, got)
    back = lax.all_to_all(partial.reshape(X * Y * ZL * C, ZH, width), near + ("c",), 0, 0, tiled=True)
    (mixed,) = call(mix_kernel, [(ZH, rows, width)], [VMEM] * 2, "mix", 6 * ZH * rows * X * slots * width, 1100000)(
        mixing, back.reshape(X, slots, width)
    )
    parts = lax.all_to_all(mixed, far, 0, 0, tiled=True)
    return jnp.sum(parts.astype(F32), axis=0).astype(BF16)


def solution(mesh):
    fine = Mesh(mesh.devices.reshape(Y, 2, 2, 2, ZL, C, X), ("y", "za", "zb", "zd", "zl", "c", "x"))
    experts = ("y", "za", "zb", "zd", "zl", "c")
    return jax.shard_map(
        shards,
        mesh=fine,
        in_specs=(
            P(experts, "x"),
            P(experts, None),
            P(experts, None),
            P(experts),
            P(experts, None, "x"),
            P(experts, "x", None),
        ),
        out_specs=P(experts, "x"),
        check_vma=False,
    )
```

```python
import jax
import jax.numpy as jnp
from jax import lax
from jax.experimental import pallas as pl
from jax.experimental.pallas import tpu as pltpu
from jax.sharding import Mesh, PartitionSpec as P

route_scale = 2.827
Y, ZH, ZL, C, X = 4, 8, 2, 2, 4
F32, BF16 = jnp.float32, jnp.bfloat16
VMEM = pl.BlockSpec(memory_space=pltpu.VMEM)
SMEM = pl.BlockSpec(memory_space=pltpu.SMEM)
HBM = pl.BlockSpec(memory_space=pltpu.HBM)
NOWHERE = 255.0
ZH_OF = (0, 4, 2, 6, 1, 5, 3, 7)


def pack_kernel(tok_hbm, ids_hbm, gate_hbm, count_ref, out_ref, tok_ref, ids_ref, gate_ref, sems):
    pairs = ((ids_hbm, ids_ref), (gate_hbm, gate_ref), (tok_hbm, tok_ref))
    copies = [pltpu.make_async_copy(src, dst, sems.at[i]) for i, (src, dst) in enumerate(pairs)]
    for copy in copies:
        copy.start()
    for copy in copies[:2]:
        copy.wait()
    rows, top = ids_ref.shape
    width = tok_ref.shape[1]
    ids = ids_ref[...]
    gate = gate_ref[...]
    high = gate.astype(BF16).astype(F32)
    mid = (gate - high).astype(BF16).astype(F32)
    low = (gate - high - mid).astype(BF16).astype(F32)
    live = lax.broadcasted_iota(jnp.int32, ids.shape, 0) < count_ref[0]
    names = jnp.where(live, ids, int(NOWHERE)).astype(F32)
    lane = lax.broadcasted_iota(jnp.int32, (rows, 128), 1)
    meta = jnp.zeros((rows, 128), F32)
    for k in range(top):
        at = slice(k, k + 1)
        for piece, part in enumerate((names, high, mid, low)):
            meta = jnp.where(lane == piece * top + k, part[:, at], meta)
    out_ref[:, width:] = meta.astype(BF16)
    copies[2].wait()
    out_ref[:, :width] = tok_ref[...]


def pick_kernel(top, in_ref, out_ref):
    width = out_ref.shape[2]
    rows = ZH * C * in_ref.shape[2]
    meta = in_ref[:, :, :, width:].astype(F32).reshape(rows, 128)
    column = lax.broadcasted_iota(jnp.int32, (rows, 128), 1)
    row = lax.broadcasted_iota(jnp.int32, (rows, 128), 0)
    own = (row // (8 * C) == column % ZH) & ((row // 8) % C == (column // ZH) % C)
    near = column // (ZH * C)
    expert = ((near // ZL) * ZH + lax.axis_index(("za", "zb", "zd"))) * (ZL * C) + (near % ZL) * C + lax.axis_index("c")
    expert = jnp.where(own, expert, -1).astype(F32)
    named = meta[:, 0:1] == expert
    for k in range(1, top):
        named = named | (meta[:, k : k + 1] == expert)
    picker = jnp.where(named, 1.0, 0.0).astype(BF16)
    tokens = in_ref[:, :, :, :width].astype(F32).reshape(rows, width).astype(BF16)
    picked = lax.dot_general(picker, tokens, (((0,), (0,)), ((), ())), preferred_element_type=F32)
    picked = picked.astype(BF16)
    for x in range(X):
        out_ref[x] = picked


def mixing_of(top, meta):
    column = lax.broadcasted_iota(jnp.int32, meta.shape, 1)
    row = lax.broadcasted_iota(jnp.int32, meta.shape, 0)
    near = column // ZH
    expert = ((near // (ZL * C)) * ZH + lax.axis_index(("za", "zb", "zd"))) * (ZL * C) + near % (ZL * C)
    expert = jnp.where(row // 8 == column % ZH, expert, -1).astype(F32)
    hits = [meta[:, k : k + 1] == expert for k in range(top)]
    total = jnp.zeros((meta.shape[0], 1), F32)
    weight = jnp.zeros(meta.shape, F32)
    for k in range(top):
        high, mid, low = (meta[:, (piece + 1) * top + k : (piece + 1) * top + k + 1] for piece in range(3))
        gate = (high + mid) + low
        total = total + gate
        weight = jnp.where(hits[k], gate, weight)
    share = route_scale * weight / total
    high = share.astype(BF16)
    mid = (share - high.astype(F32)).astype(BF16)
    low = (share - high.astype(F32) - mid.astype(F32)).astype(BF16)
    return [high, mid, low]


def expert_kernel(top, in_ref, up_ref, down_ref, meta_ref, out_ref, mixing_ref):
    width = in_ref.shape[2]
    raised = None
    for x in range(X):
        term = jnp.dot(in_ref[x], up_ref[0, x * width : (x + 1) * width, :], preferred_element_type=F32)
        raised = term if raised is None else raised + term
    rows = ZH * meta_ref.shape[2]
    meta = meta_ref[:, lax.axis_index("c"), :, width:].astype(F32).reshape(rows, 128)
    for piece, weight in enumerate(mixing_of(top, meta)):
        mixing_ref[piece * rows : (piece + 1) * rows] = weight
    hidden = (raised / (1.0 + jnp.exp(-raised))).astype(BF16)
    for x in range(X):
        lowered = jnp.dot(hidden, down_ref[0, :, x * width : (x + 1) * width], preferred_element_type=F32)
        out_ref[x] = lowered.astype(BF16)


def mix_kernel(mixing_ref, in_ref, out_ref):
    rows = mixing_ref.shape[0] // 3
    wide = jnp.concatenate([mixing_ref[...]] * X, axis=1)
    slots, width = in_ref.shape[1:]
    total = jnp.dot(wide, in_ref[...].reshape(X * slots, width), preferred_element_type=F32)
    mixed = (total[2 * rows :] + total[rows : 2 * rows]) + total[:rows]
    for to in range(ZH):
        out_ref[to] = mixed[ZH_OF[to] * 8 : ZH_OF[to] * 8 + 8].astype(BF16)


def call(kernel, out_shape, specs, name, flops, bytes_accessed, scratch=()):
    return pl.pallas_call(
        kernel,
        out_shape=[jax.ShapeDtypeStruct(shape, BF16) for shape in out_shape],
        in_specs=specs,
        out_specs=[VMEM] * len(out_shape),
        scratch_shapes=list(scratch),
        name=name,
        compiler_params=pltpu.CompilerParams(vmem_limit_bytes=16 * 1024 * 1024),
        cost_estimate=pl.CostEstimate(flops=flops, bytes_accessed=bytes_accessed, transcendentals=0),
    )


def in_hbm(array):
    return pltpu.with_memory_space_constraint(array, pltpu.HBM)


def shards(tokens, expert_ids, gate_weight, valid_count, up_weight, down_weight):
    rows, width = tokens.shape
    top = expert_ids.shape[1]
    hidden = up_weight.shape[2]
    far, near = ("zd", "zb", "za"), ("x", "y", "zl")
    slots = Y * ZL * C * ZH
    (packed,) = call(
        pack_kernel,
        [(rows, width + 128)],
        [HBM] * 3 + [SMEM],
        "pack",
        100000,
        200000,
        [
            pltpu.VMEM(tokens.shape, BF16),
            pltpu.VMEM(expert_ids.shape, jnp.int32),
            pltpu.VMEM(gate_weight.shape, F32),
            pltpu.SemaphoreType.DMA((3,)),
        ],
    )(in_hbm(tokens), in_hbm(expert_ids), in_hbm(gate_weight), valid_count)
    got = lax.all_gather(packed, ("za", "zb", "zd", "c"), axis=0, tiled=False).reshape(ZH, C, rows, width + 128)
    (picked,) = call(lambda *refs: pick_kernel(top, *refs), [(X, slots, width)], [VMEM], "pick", 4 * 10**9, 1100000)(got)
    routed = lax.all_to_all(picked.reshape(X * Y * ZL, C * ZH, width), near, 0, 0, tiled=True)
    partial, mixing = call(
        lambda *refs: expert_kernel(top, *refs),
        [(X, slots, width), (3 * ZH * rows, slots)],
        [VMEM] * 4,
        "expert",
        4 * slots * X * width * hidden,
        5000000,
    )(routed.reshape(X, slots, width), up_weight, down_weight, got)
    back = lax.all_to_all(partial.reshape(X * Y * ZL * C, ZH, width), near + ("c",), 0, 0, tiled=True)
    (mixed,) = call(mix_kernel, [(ZH, rows, width)], [VMEM] * 2, "mix", 6 * ZH * rows * X * slots * width, 1100000)(
        mixing, back.reshape(X, slots, width)
    )
    parts = lax.all_to_all(mixed, far, 0, 0, tiled=True)
    return jnp.sum(parts.astype(F32), axis=0).astype(BF16)


def solution(mesh):
    fine = Mesh(mesh.devices.reshape(Y, 2, 2, 2, ZL, C, X), ("y", "za", "zb", "zd", "zl", "c", "x"))
    experts = ("y", "za", "zb", "zd", "zl", "c")
    return jax.shard_map(
        shards,
        mesh=fine,
        in_specs=(
            P(experts, "x"),
            P(experts, None),
            P(experts, None),
            P(experts),
            P(experts, None, "x"),
            P(experts, "x", None),
        ),
        out_specs=P(experts, "x"),
        check_vma=False,
    )
```
